512 devices in a mesh: seq: 32 (over x_lo, y, core), head: 16 (over z, x_hi).
Axes of the slice: x: 4 (x_hi: 2, x_lo: 2; x = x_hi * 2 + x_lo), y: 8, z: 8, core: 2. Of those that a mesh axis runs over, the one named last changes fastest.
Arguments:
- lat_query: bfloat16 [4096, 73728], P('seq', 'head'), may hold values from -6 to 6
- lat_keys: bfloat16 [4096, 576], P('seq'), may hold values from -6 to 6
- normalizer: float32 [4096, 128], P('seq'), may hold values from 3 to 7
- lookback: int32 [4096], P('seq'), may hold values from 1 to 4096
- index_query: bfloat16 [4096, 8192], P(('seq', 'head')), may hold values from -20 to 20
- index_keys: bfloat16 [4096, 128], P('seq'), may hold values from -6 to 6
- index_weight: float32 [4096, 64], P(('seq', 'head')), may hold values from 0.25 to 2
Outputs:
- grad_query: float32 [4096, 8192], P(('seq', 'head'))
- grad_weight: float32 [4096, 64], P(('seq', 'head'))
- grad_key: float32 [4096, 128], P(('seq', 'head'))
The draws below stay inside these ranges and needn't reach their ends.
All inputs are finite; a program needn't handle non-finite values.
Results may differ from the reference program's by a relative error of at most 0.0029.
Values may be sent and summed in bfloat16 or wider, within the bound.
A program may use at most 64 MiB of HBM per device.

```python
import math
import jax
import jax.numpy as jnp
from jax import lax

HEADS = 128
KDIM = 576
IHEADS = 64
IDIM = 128
SEQ_LEN = 4096


def index_pair(key):
    base_key = jax.random.fold_in(key, 7101)
    key_values = jnp.clip(jax.random.normal(jax.random.fold_in(base_key, 1), (SEQ_LEN, IDIM), jnp.float32), -5.0, 5.0)
    query_values = jnp.clip(jax.random.normal(jax.random.fold_in(base_key, 2), (SEQ_LEN, IHEADS, IDIM), jnp.float32), -5.0, 5.0)
    return (query_values.reshape(SEQ_LEN, IHEADS * IDIM), key_values)


def draw_index_query(key, part):
    return index_pair(key)[0].astype(jnp.bfloat16)


def draw_index_keys(key, part):
    return index_pair(key)[1].astype(jnp.bfloat16)


def plant(drawn, own_key, low, high):
    extent = drawn.shape
    index_at = [jax.random.randint(jax.random.fold_in(own_key, axis), (), 0, extent[axis]) for axis in range(len(extent))]
    drawn = drawn.at[tuple(index_at)].set(low)
    longest = extent.index(max(extent))
    index_at[longest] = (index_at[longest] + 1) % extent[longest]
    return drawn.at[tuple(index_at)].set(high)


def steps_of(stream_key, extent, split, low, largest):
    def one(position, shards_of):
        steps = jax.random.uniform(jax.random.fold_in(jax.random.fold_in(stream_key, 6), position), (shards_of,), jnp.float32, low / len(split), largest / len(split))
        return jnp.repeat(jnp.exp(steps), extent[position] // shards_of).reshape((-1,) + (1,) * (len(extent) - position - 1))

    gain = one(*split[0])
    for cut in split[1:]:
        gain = gain * one(*cut)
    return gain


def gaussian(stream_key, dims, deviation, most, cuts=(), kind=jnp.bfloat16):
    result = deviation * jax.random.normal(stream_key, dims, jnp.float32)
    if cuts:
        result = result * steps_of(stream_key, dims, cuts, -0.22, 0.18)
    return jnp.clip(result, -most, most).astype(kind)


def setup_inputs(seed: int = 0) -> dict:
    seeds = jax.random.split(jax.random.key(seed), 8)
    return {
        "lat_query": gaussian(seeds[0], (SEQ_LEN, HEADS * KDIM), 1.0, 6.0, ((0, 32), (1, 16))),
        "lat_keys": gaussian(seeds[1], (SEQ_LEN, KDIM), 1.0, 6.0, ((0, 32),)),
        "normalizer": jnp.clip(3.0 + 4.0 * jax.random.uniform(seeds[2], (SEQ_LEN, HEADS), jnp.float32) ** steps_of(seeds[2], (SEQ_LEN, HEADS), ((0, 32),), -0.2, 0.2), 3.0, 7.0),
        "lookback": plant(jax.random.randint(seeds[3], (SEQ_LEN,), 1, SEQ_LEN + 1), jax.random.fold_in(seeds[3], 1), 1, SEQ_LEN).astype(jnp.int32),
        "index_query": draw_index_query(jax.random.fold_in(seeds[7], 71), 0),
        "index_keys": draw_index_keys(jax.random.fold_in(seeds[7], 71), 0),
        "index_weight": jnp.clip(jnp.exp(math.log(2.0) - 2.0794415 * jax.random.uniform(seeds[6], (SEQ_LEN, IHEADS), jnp.float32) ** steps_of(seeds[6], (SEQ_LEN, IHEADS), ((0, 512),), -0.2, 0.2)), 0.25, 2.0),
    }


def index_pass(query, weight, target, key_rows, row_pos, row_low):
    row_count = query.shape[0]
    head_count = weight.shape[1]
    key_depth = key_rows.shape[1]
    seq_total = key_rows.shape[0]
    block_rows = min(512, seq_total)
    blocks = seq_total // block_rows
    flat_query = query.reshape(row_count * head_count, key_depth)
    flat_weight = weight.reshape(row_count * head_count)
    factor = key_depth ** -0.5

    def scores(block_index):
        key_part = lax.dynamic_slice_in_dim(key_rows, block_index * block_rows, block_rows, 0)
        inner = lax.dot_general(flat_query, key_part, (((1,), (1,)), ((), ())), preferred_element_type=jnp.float32) * factor
        active = jnp.maximum(inner, 0.0)
        summed = jnp.sum((active * flat_weight[:, None]).reshape(row_count, head_count, block_rows), axis=1)
        key_pos = block_index * block_rows + jnp.arange(block_rows, dtype=jnp.int32)
        visible = (key_pos[None, :] <= row_pos[:, None]) & (key_pos[None, :] >= row_low[:, None])
        return key_part, inner, active, summed, visible

    def first_pass(running, block_index):
        row_top, row_mass = running
        _, _, _, summed, visible = scores(block_index)
        summed = jnp.where(visible, summed, -jnp.inf)
        new_top = jnp.maximum(row_top, jnp.max(summed, axis=1))
        row_mass = row_mass * jnp.exp(row_top - new_top) + jnp.sum(jnp.exp(summed - new_top[:, None]), axis=1)
        return (new_top, row_mass), None

    start_state = (jnp.full((row_count,), -1e30, jnp.float32), jnp.zeros((row_count,), jnp.float32))
    (row_top, row_mass), _ = lax.scan(first_pass, start_state, jnp.arange(blocks, dtype=jnp.int32))

    def second_pass(running, block_index):
        d_query, d_weight = running
        key_part, inner, active, summed, visible = scores(block_index)
        predicted = jnp.where(visible, jnp.exp(summed - row_top[:, None]) / row_mass[:, None], 0.0)
        target_block = lax.dynamic_slice_in_dim(target, block_index * block_rows, block_rows, 1)
        gap_term = predicted - target_block
        d_weight = d_weight + jnp.sum(active.reshape(row_count, head_count, block_rows) * gap_term[:, None, :], axis=2)
        spread = (gap_term[:, None, :] * weight[:, :, None]).reshape(row_count * head_count, block_rows) * factor
        slopes = jnp.where(inner > 0, spread, 0.0).astype(jnp.bfloat16)
        d_query = d_query + jnp.dot(slopes, key_part, preferred_element_type=jnp.float32)
        d_key = lax.dot_general(slopes, flat_query, (((0,), (0,)), ((), ())), preferred_element_type=jnp.float32)
        return (d_query, d_weight), d_key

    start_grads = (jnp.zeros((row_count * head_count, key_depth), jnp.float32), jnp.zeros((row_count, head_count), jnp.float32))
    (d_query, d_weight), d_key = lax.scan(second_pass, start_grads, jnp.arange(blocks, dtype=jnp.int32))
    return d_query.reshape(row_count, head_count * key_depth), d_weight, d_key.reshape(seq_total, key_depth)


def attention_mass(lat_query, lat_keys, normalizer, lookback):
    seq_total = lat_query.shape[0]
    block_rows = min(512, seq_total)
    score_scale = KDIM ** -0.5
    key_full = lat_keys.astype(jnp.float32)
    pieces = []
    for block_index in range(seq_total // block_rows):
        begin = block_index * block_rows
        finish = begin + block_rows
        query_block = lat_query[begin:finish].reshape(block_rows, HEADS, KDIM).astype(jnp.float32)
        query_block = jnp.transpose(query_block, (1, 0, 2))
        offsets = jnp.transpose(normalizer[begin:finish])
        key_block = key_full[:finish]

        def head_step(summed, inputs):
            query_head, offset_head = inputs
            scores = jnp.dot(query_head, key_block.T, preferred_element_type=jnp.float32, precision=lax.Precision.HIGHEST)
            return summed + jnp.exp(scores * score_scale - offset_head[:, None]), None

        summed, _ = lax.scan(head_step, jnp.zeros((block_rows, finish), jnp.float32), (query_block, offsets))
        query_pos = begin + jnp.arange(block_rows, dtype=jnp.int32)
        query_low = query_pos - lookback[begin:finish]
        key_pos = jnp.arange(finish, dtype=jnp.int32)
        visible = (key_pos[None, :] <= query_pos[:, None]) & (key_pos[None, :] >= query_low[:, None])
        summed = jnp.where(visible, summed, 0.0)
        pieces.append(jnp.concatenate([summed, jnp.zeros((block_rows, seq_total - finish), jnp.float32)], axis=1))
    return jnp.concatenate(pieces, axis=0)


def reference(lat_query, lat_keys, normalizer, lookback, index_query, index_keys, index_weight):
    seq_total = lat_query.shape[0]
    mass = attention_mass(lat_query, lat_keys, normalizer, lookback)
    target = mass / jnp.sum(mass, axis=1, keepdims=True)
    group_rows = min(64, seq_total)
    positions = jnp.arange(seq_total, dtype=jnp.int32)
    lows = positions - lookback

    def group_step(key_sum, group_index):
        begin = (group_index * group_rows).astype(jnp.int32)
        query_rows = lax.dynamic_slice_in_dim(index_query, begin, group_rows, 0)
        weight_rows = lax.dynamic_slice_in_dim(index_weight, begin, group_rows, 0)
        target_rows = lax.dynamic_slice_in_dim(target, begin, group_rows, 0)
        pos_rows = lax.dynamic_slice_in_dim(positions, begin, group_rows, 0)
        low_rows = lax.dynamic_slice_in_dim(lows, begin, group_rows, 0)
        d_query, d_weight, d_key = index_pass(query_rows, weight_rows, target_rows, index_keys, pos_rows, low_rows)
        return key_sum + d_key, (d_query, d_weight)

    key_sum, (d_query, d_weight) = lax.scan(group_step, jnp.zeros((seq_total, IDIM), jnp.float32), jnp.arange(seq_total // group_rows, dtype=jnp.int32))
    return d_query.reshape(seq_total, IHEADS * IDIM), d_weight.reshape(seq_total, IHEADS), key_sum
```

```python
import functools
import math

import jax
import jax.numpy as jnp
from jax import lax
from jax.experimental import pallas as pl
from jax.experimental.pallas import tpu as pltpu
from jax.sharding import PartitionSpec as P

F32 = jnp.float32
BF16 = jnp.bfloat16
KDIM = 576
KPAD = 640
IDIM = 128
IHEADS = 64
NX_LO, NY, NCORE = 2, 8, 2
NZ, NX_HI = 8, 2
SLOTS = NX_LO * NY * NCORE
ROWS = 128
HALF = ROWS // 2
OWN = 8
QROWS = 16
LOCAL_HEADS = 8
CH = 256
NCH = SLOTS * ROWS // CH
LOG2E = math.log2(math.e)
SCORE_SCALE = KDIM ** (-0.5)
FACTOR = IDIM ** (-0.5)
MESH = pl.DeviceIdType.MESH


def kernel(
    lq_ref, lk_ref, norm_ref, look_ref, iq_ref, ik_ref, iw_ref,
    gq_ref, gw_ref, gk_ref,
    qrecv, qmat, keys, nbc, wbc, iqf, iqb, iqt, inner, pred, mpart, mrecv,
    dqa, dwa, dkey, r1recv, pz, py, rz, ry, sz, sy, r3z, r3y, tx, r4,
    q_ss, q_rs, k_ss, k_rs, m_ss, m_rs, r1_ss, r1_rs,
    z2_ss, z2_rs, y2_ss, y2_rs, z3_ss, z3_rs, y3_ss, y3_rs, x4_ss, x4_rs, loc_sem,
):
    s = lax.axis_index("seq")
    h = lax.axis_index("head")
    core = s % 2
    y = (s // 2) % NY
    x_lo = s // (2 * NY)
    x_hi = h % 2
    z = h // 2

    def slot(xl, yy, cc):
        return (xl * NY + yy) * 2 + cc

    def dev(xl, yy, cc, zz, xh):
        return (slot(xl, yy, cc), zz * 2 + xh)

    def at_z(d):
        return dev(x_lo, y, core, (z + d) % NZ, x_hi)

    def at_y(d):
        return dev(x_lo, (y + d) % NY, core, z, x_hi)

    other_core = dev(x_lo, y, 1 - core, z, x_hi)
    x_near = dev(1 - x_lo, y, core, z, x_hi)
    x_far = dev(1 - x_lo, y, core, z, 1 - x_hi)
    x_two = dev(x_lo, y, core, z, 1 - x_hi)

    keys[s, :, :KDIM] = lk_ref[...]
    keys[s, :, KDIM:KPAD] = jnp.zeros((ROWS, KPAD - KDIM), BF16)
    keys[s, :, KPAD:] = ik_ref[...]

    barrier = pltpu.get_barrier_semaphore()
    peers = [at_z(d) for d in range(1, NZ)] + [at_y(d) for d in range(1, NY)]
    peers += [other_core, x_near, x_far, x_two]
    for peer in peers:
        pl.semaphore_signal(barrier, inc=1, device_id=peer, device_id_type=MESH)
    pl.semaphore_wait(barrier, len(peers))

    sent = []

    def remote(src, dst, ss, rs, peer):
        return pltpu.make_async_remote_copy(
            src_ref=src, dst_ref=dst, send_sem=ss, recv_sem=rs, device_id=peer, device_id_type=MESH
        )

    def half_ref(sl, half):
        return keys.at[sl, pl.ds(half * HALF, HALF), :]

    count = [0]

    def send_key(sl, half, peer):
        n = count[0]
        count[0] += 1
        cp = remote(half_ref(sl, half), half_ref(sl, half), k_ss.at[n], k_rs.at[sl, half], peer)
        cp.start()
        sent.append(cp)

    def wait_key(sl, half):
        ref = half_ref(sl, half)
        remote(ref, ref, k_ss.at[0], k_rs.at[sl, half], other_core).wait_recv()

    right, left = at_y(1), at_y(NY - 1)
    for half in range(2):
        send_key(s, half, right)
        send_key(s, half, left)
        send_key(s, half, (x_near, x_far)[half])
    for d in (4, 3, 5, 2, 6, 1, 7):
        cp = remote(lq_ref.at[(z + d) % NZ], qrecv.at[d], q_ss.at[d], q_rs.at[d], at_z(d))
        cp.start()
        sent.append(cp)
    for half in range(2):
        send_key(s, half, other_core)
    own_q = pltpu.make_async_copy(lq_ref.at[z], qrecv.at[0], loc_sem)
    own_q.start()

    lane = lax.broadcasted_iota(jnp.int32, (OWN, 128), 1)
    row = lax.broadcasted_iota(jnp.int32, (OWN, 128), 0)
    look = jnp.sum(
        jnp.where(lane == h * OWN + row, jnp.broadcast_to(look_ref[...], (OWN, 128)), 0),
        axis=1, keepdims=True,
    )
    query_pos = s * ROWS + h * OWN + lax.broadcasted_iota(jnp.int32, (OWN, 1), 0)
    query_low = query_pos - look
    iq32 = iq_ref[...].astype(F32)
    iw = iw_ref[...] * FACTOR
    for j in range(IHEADS):
        iqf[j * OWN : (j + 1) * OWN, :] = iq32[:, j * IDIM : (j + 1) * IDIM]
        wbc[j * OWN : (j + 1) * OWN, :] = jnp.broadcast_to(iw[:, j : j + 1], (OWN, CH))
    iqb[...] = iqf[...].astype(BF16)
    iqt[...] = iqf[...].T.astype(BF16)

    def on_y(k, half, going_right):
        yy = (y + NY - k) % NY if going_right else (y + k) % NY
        sl = slot(x_lo, yy, core)
        wait_key(sl, half)
        if k < 3 or (k == 3 and half == (0 if going_right else 1)):
            send_key(sl, half, right if going_right else left)
        send_key(sl, half, (x_near, x_far)[half])
        send_key(sl, half, other_core)

    def on_x(yy):
        sl = slot(1 - x_lo, yy, core)
        for half in range(2):
            wait_key(sl, half)
            send_key(sl, half, other_core)

    for k in range(1, 5):
        if k < 4:
            for half in range(2):
                on_y(k, half, True)
                on_y(k, half, False)
        else:
            on_y(4, 0, True)
            on_y(4, 1, False)
        on_x((y + NY - k + 1) % NY)
        if k > 1:
            on_x((y + k - 1) % NY)
    on_x((y + 4) % NY)

    nrm = norm_ref[pl.ds(pl.multiple_of(z * QROWS, QROWS), QROWS), :] * LOG2E
    lane16 = lax.broadcasted_iota(jnp.int32, (QROWS, 128), 1)
    for d in range(NZ):
        first = (((z + NZ - d) % NZ) * 2 + x_hi) * LOCAL_HEADS
        for g in range(LOCAL_HEADS):
            col = jnp.sum(jnp.where(lane16 == first + g, nrm, 0.0), axis=1, keepdims=True)
            at = (d * LOCAL_HEADS + g) * QROWS
            nbc[at : at + QROWS, :] = jnp.broadcast_to(col, (QROWS, CH))

    def wait_core(p, carry):
        sl = p * 2 + 1 - core
        for half in range(2):
            wait_key(sl, half)
        return carry

    lax.fori_loop(0, NX_LO * NY, wait_core, 0)

    def visible(j):
        key_pos = j * CH + lax.broadcasted_iota(jnp.int32, (OWN, CH), 1)
        return (key_pos <= query_pos) & (key_pos >= query_low)

    def score_step(j, top):
        kk = keys[pl.ds(2 * j, 2), :, KPAD:].reshape(CH, IDIM)
        raw = lax.dot_general(
            iqb[...], kk, (((1,), (1,)), ((), ())), preferred_element_type=F32
        )
        inner[j] = raw
        act = jnp.maximum(raw, 0.0) * wbc[...]
        score = jnp.sum(act.reshape(IHEADS, OWN, CH), axis=0)
        score = jnp.where(visible(j), score, -jnp.inf)
        pred[j] = score
        return jnp.maximum(top, score)

    top = lax.fori_loop(0, NCH, score_step, jnp.full((OWN, CH), -jnp.inf, F32))
    top = jnp.max(top, axis=1, keepdims=True)
    p_all = jnp.exp(pred[...] - top[None])
    p_sum = jnp.sum(jnp.sum(p_all, axis=0), axis=1, keepdims=True)
    pred[...] = p_all / p_sum[None]

    own_q.wait()
    for d in (0, 1, 7, 2, 6, 3, 5, 4):
        if d:
            remote(qrecv.at[d], qrecv.at[d], q_ss.at[d], q_rs.at[d], at_z(d)).wait_recv()
        for p in range(LOCAL_HEADS // 2):
            at = (d * LOCAL_HEADS + 2 * p) * QROWS
            base = 2 * p * KDIM
            qmat[at : at + QROWS, :] = qrecv[d, :, base : base + KPAD]
            odd = qrecv[d, :, base + 512 : base + 512 + KPAD].astype(F32)
            odd = pltpu.roll(odd, KPAD - 64, 1)
            qmat[at + QROWS : at + 2 * QROWS, :] = odd.astype(BF16)

    GROUP = 256

    def mass_step(j, carry):
        kk = keys[pl.ds(2 * j, 2), :, :KPAD].reshape(CH, KPAD)
        total = jnp.zeros((QROWS, CH), F32)
        for q in range(4):
            sc = lax.dot_general(
                qmat[q * GROUP : (q + 1) * GROUP, :], kk, (((1,), (1,)), ((), ())),
                preferred_element_type=F32,
            )
            ex = jnp.exp2(sc * (SCORE_SCALE * LOG2E) - nbc[q * GROUP : (q + 1) * GROUP, :])
            total = total + jnp.sum(ex.reshape(GROUP // QROWS, QROWS, CH), axis=0)
        mpart[j] = total.reshape(2, OWN, CH)
        return carry

    for c in range(4):
        lax.fori_loop(4 * c, 4 * c + 4, mass_step, 0)
        cp = remote(
            mpart.at[pl.ds(4 * c, 4), 1 - x_hi], mrecv.at[pl.ds(4 * c, 4)],
            m_ss.at[c], m_rs.at[c], x_two,
        )
        cp.start()
        sent.append(cp)
    for c in range(4):
        remote(
            mpart.at[pl.ds(4 * c, 4), 1 - x_hi], mrecv.at[pl.ds(4 * c, 4)],
            m_ss.at[c], m_rs.at[c], x_two,
        ).wait_recv()

    def mass_sum(j, acc):
        m = jnp.where(visible(j), mpart[j, x_hi] + mrecv[j], 0.0)
        mrecv[j] = m
        return acc + m

    mass = lax.fori_loop(0, NCH, mass_sum, jnp.zeros((OWN, CH), F32))
    mass = jnp.sum(mass, axis=1, keepdims=True)

    dqa[...] = jnp.zeros_like(dqa)
    dwa[...] = jnp.zeros_like(dwa)

    def r1_copy(j):
        return remote(dkey.at[j, 1 - core], r1recv.at[j], r1_ss.at[j], r1_rs.at[j], other_core)

    def grad_step(j, carry):
        gap = pred[j] - mrecv[j] / mass
        raw = inner[j].reshape(IHEADS, OWN, CH)
        act = jnp.maximum(raw, 0.0) * gap[None]
        act = act.reshape(IHEADS * OWN, CH)
        dwa[...] += act[:, :128] + act[:, 128:]
        slope = jnp.where(raw > 0, gap[None] * wbc[...].reshape(IHEADS, OWN, CH), 0.0)
        slope = slope.reshape(IHEADS * OWN, CH).astype(BF16)
        kk = keys[pl.ds(2 * j, 2), :, KPAD:].reshape(CH, IDIM)
        dqa[...] += jnp.dot(slope, kk, preferred_element_type=F32)
        dk = jnp.dot(iqt[...], slope, preferred_element_type=F32)
        dkey[j] = dk.T.reshape(2, ROWS, IDIM)
        r1_copy(j).start()
        return carry

    lax.fori_loop(0, NCH, grad_step, 0)

    def r1_sum(xl):
        def step(yy, carry):
            j = xl * NY + yy
            r1_copy(j).wait_recv()
            both = dkey[j, core] + r1recv[j]
            parts = both.reshape(NZ, 2, OWN, IDIM)
            pz[:, yy, xl] = parts[:, 0]
            py[yy, :, xl] = parts[:, 1]
            return carry

        lax.fori_loop(0, NY, step, 0)

    for xl in range(NX_LO):
        r1_sum(xl)

    order = (4, 3, 5, 2, 6, 1, 7)
    for d in order:
        for cp in (
            remote(pz.at[(z + d) % NZ], rz.at[d], z2_ss.at[d], z2_rs.at[d], at_z(d)),
            remote(py.at[(y + d) % NY], ry.at[d], y2_ss.at[d], y2_rs.at[d], at_y(d)),
        ):
            cp.start()
            sent.append(cp)

    lane_w = lax.broadcasted_iota(jnp.int32, (OWN, 128), 1)
    gw = jnp.zeros((OWN, 128), F32)
    for j in range(IHEADS):
        gq_ref[:, j * IDIM : (j + 1) * IDIM] = dqa[j * OWN : (j + 1) * OWN, :]
        col = jnp.sum(dwa[j * OWN : (j + 1) * OWN, :], axis=1, keepdims=True)
        gw = jnp.where(lane_w == j, jnp.broadcast_to(col, (OWN, 128)), gw)
    gw_ref[...] = gw[:, :IHEADS] * FACTOR

    az, ay = pz[z], py[y]
    for d in (1, 7, 2, 6, 3, 5, 4):
        remote(pz.at[d], rz.at[d], z2_ss.at[d], z2_rs.at[d], at_z(d)).wait_recv()
        remote(py.at[d], ry.at[d], y2_ss.at[d], y2_rs.at[d], at_y(d)).wait_recv()
        az = az + rz[d]
        ay = ay + ry[d]
    sz[...] = az
    sy[...] = ay
    for d in order:
        for cp in (
            remote(sz.at[(y + d) % NY], r3z.at[d], y3_ss.at[d], y3_rs.at[d], at_y(d)),
            remote(sy.at[(z + d) % NZ], r3y.at[d], z3_ss.at[d], z3_rs.at[d], at_z(d)),
        ):
            cp.start()
            sent.append(cp)
    t0, t1 = sz[y], sy[z]
    for d in (1, 7, 2, 6, 3, 5, 4):
        remote(sz.at[d], r3z.at[d], y3_ss.at[d], y3_rs.at[d], at_y(d)).wait_recv()
        remote(sy.at[d], r3y.at[d], z3_ss.at[d], z3_rs.at[d], at_z(d)).wait_recv()
        t0 = t0 + r3z[d]
        t1 = t1 + r3y[d]
    tx[0] = t0
    tx[1] = t1
    last = []
    for n, (peer, xh, xl) in enumerate(
        ((x_near, x_hi, 1 - x_lo), (x_far, 1 - x_hi, 1 - x_lo), (x_two, 1 - x_hi, x_lo))
    ):
        cp = remote(tx.at[xh, xl], r4.at[n], x4_ss.at[n], x4_rs.at[n], peer)
        cp.start()
        sent.append(cp)
        last.append(cp)
    out = tx[x_hi, x_lo]
    for n, cp in enumerate(last):
        cp.wait_recv()
        out = out + r4[n]
    gk_ref[...] = out

    for cp in sent:
        cp.wait_send()

    def r1_done(j, carry):
        r1_copy(j).wait_send()
        return carry

    lax.fori_loop(0, NCH, r1_done, 0)


def per_device(lat_query, lat_keys, normalizer, lookback, index_query, index_keys, index_weight):
    vmem = pl.BlockSpec(memory_space=pltpu.VMEM)
    dma = pltpu.SemaphoreType.DMA
    return pl.pallas_call(
        kernel,
        out_shape=(
            jax.ShapeDtypeStruct((OWN, IHEADS * IDIM), F32),
            jax.ShapeDtypeStruct((OWN, IHEADS), F32),
            jax.ShapeDtypeStruct((OWN, IDIM), F32),
        ),
        in_specs=[pl.BlockSpec(memory_space=pl.ANY)] + [vmem] * 6,
        out_specs=(vmem, vmem, vmem),
        scratch_shapes=[
            pltpu.VMEM((NZ, QROWS, LOCAL_HEADS * KDIM), BF16),
            pltpu.VMEM((NZ * LOCAL_HEADS * QROWS, KPAD), BF16),
            pltpu.VMEM((SLOTS, ROWS, KPAD + IDIM), BF16),
            pltpu.VMEM((NZ * LOCAL_HEADS * QROWS, CH), F32),
            pltpu.VMEM((IHEADS * OWN, CH), F32),
            pltpu.VMEM((IHEADS * OWN, IDIM), F32),
            pltpu.VMEM((IHEADS * OWN, IDIM), BF16),
            pltpu.VMEM((IDIM, IHEADS * OWN), BF16),
            pltpu.VMEM((NCH, IHEADS * OWN, CH), F32),
            pltpu.VMEM((NCH, OWN, CH), F32),
            pltpu.VMEM((NCH, 2, OWN, CH), F32),
            pltpu.VMEM((NCH, OWN, CH), F32),
            pltpu.VMEM((IHEADS * OWN, IDIM), F32),
            pltpu.VMEM((IHEADS * OWN, 128), F32),
            pltpu.VMEM((NCH, 2, ROWS, IDIM), F32),
            pltpu.VMEM((NCH, ROWS, IDIM), F32),
            pltpu.VMEM((NZ, NY, NX_LO, OWN, IDIM), F32),
            pltpu.VMEM((NY, NZ, NX_LO, OWN, IDIM), F32),
            pltpu.VMEM((NZ, NY, NX_LO, OWN, IDIM), F32),
            pltpu.VMEM((NY, NZ, NX_LO, OWN, IDIM), F32),
            pltpu.VMEM((NY, NX_LO, OWN, IDIM), F32),
            pltpu.VMEM((NZ, NX_LO, OWN, IDIM), F32),
            pltpu.VMEM((NY, NX_LO, OWN, IDIM), F32),
            pltpu.VMEM((NZ, NX_LO, OWN, IDIM), F32),
            pltpu.VMEM((NX_HI, NX_LO, OWN, IDIM), F32),
            pltpu.VMEM((3, OWN, IDIM), F32),
            dma((NZ,)), dma((NZ,)), dma((64,)), dma((SLOTS, 2)), dma((4,)), dma((4,)),
            dma((NCH,)), dma((NCH,)),
            dma((NZ,)), dma((NZ,)), dma((NY,)), dma((NY,)),
            dma((NZ,)), dma((NZ,)), dma((NY,)), dma((NY,)),
            dma((3,)), dma((3,)), dma,
        ],
        compiler_params=pltpu.CompilerParams(
            collective_id=0, has_side_effects=True, vmem_limit_bytes=56 << 20
        ),
    )(
        lat_query.reshape(NZ, QROWS, LOCAL_HEADS * KDIM),
        lat_keys,
        normalizer,
        lookback.reshape(1, ROWS),
        index_query,
        index_keys,
        index_weight,
    )


def solution(mesh):
    return jax.shard_map(
        per_device,
        mesh=mesh,
        in_specs=(
            P("seq", "head"),
            P("seq", None),
            P("seq", None),
            P("seq"),
            P(("seq", "head"), None),
            P("seq", None),
            P(("seq", "head"), None),
        ),
        out_specs=(P(("seq", "head"), None), P(("seq", "head"), None), P(("seq", "head"), None)),
        check_vma=False,
    )
```

```python
import functools
import math

import jax
import jax.numpy as jnp
from jax import lax
from jax.experimental import pallas as pl
from jax.experimental.pallas import tpu as pltpu
from jax.sharding import PartitionSpec as P

F32 = jnp.float32
BF16 = jnp.bfloat16
KDIM = 576
KPAD = 640
IDIM = 128
IHEADS = 64
NX_LO, NY, NCORE = 2, 8, 2
NZ, NX_HI = 8, 2
SLOTS = NX_LO * NY * NCORE
ROWS = 128
HALF = ROWS // 2
OWN = 8
QROWS = 16
LOCAL_HEADS = 8
CH = 256
NCH = SLOTS * ROWS // CH
LOG2E = math.log2(math.e)
SCORE_SCALE = KDIM ** (-0.5)
FACTOR = IDIM ** (-0.5)
MESH = pl.DeviceIdType.MESH
SLABS = (0, 4, 3, 5, 2, 6, 1, 7)
FAR_FIRST = (4, 3, 5, 2, 6, 1, 7)
GROUP = 256
OUT_W = IHEADS * IDIM


def kernel(
    lq_ref, lk_ref, norm_ref, look_ref, iq_ref, ik_ref, iw_ref,
    out_ref,
    qrecv, qmat, keys, nbc, wbc, iqf, iqb, iqt, inner, pred, mpart, mrecv,
    dqa, dwa, slp, dkey, r1recv, pz, py, rz, ry, sz, sy, r3z, r3y, tx, r4,
    q_ss, q_rs, k_ss, k_rs, m_ss, m_rs, r1_ss, r1_rs,
    z2_ss, z2_rs, y2_ss, y2_rs, z3_ss, z3_rs, y3_ss, y3_rs, x4_ss, x4_rs, loc_sem,
):
    s = lax.axis_index("seq")
    h = lax.axis_index("head")
    core = s % 2
    y = (s // 2) % NY
    x_lo = s // (2 * NY)
    x_hi = h % 2
    z = h // 2

    def slot(xl, yy, cc):
        return (xl * NY + yy) * 2 + cc

    def dev(xl, yy, cc, zz, xh):
        return (slot(xl, yy, cc), zz * 2 + xh)

    def at_z(d):
        return dev(x_lo, y, core, (z + d) % NZ, x_hi)

    def at_y(d):
        return dev(x_lo, (y + d) % NY, core, z, x_hi)

    other_core = dev(x_lo, y, 1 - core, z, x_hi)
    x_near = dev(1 - x_lo, y, core, z, x_hi)
    x_far = dev(1 - x_lo, y, core, z, 1 - x_hi)
    x_two = dev(x_lo, y, core, z, 1 - x_hi)

    barrier = pltpu.get_barrier_semaphore()
    peers = [at_z(d) for d in range(1, NZ)] + [at_y(d) for d in range(1, NY)]
    peers += [other_core, x_near, x_far, x_two]
    for peer in peers:
        pl.semaphore_signal(barrier, inc=1, device_id=peer, device_id_type=MESH)

    for i in range(4):
        part = lk_ref[i * 128 : (i + 1) * 128, :].astype(F32)
        keys[s, :, i * 128 : (i + 1) * 128] = part.T.astype(BF16)
    part = jnp.concatenate(
        [lk_ref[512:KDIM, :].astype(F32), jnp.zeros((KPAD - KDIM, ROWS), F32)], axis=0
    )
    keys[s, :, 512:KPAD] = part.T.astype(BF16)
    keys[s, :, KPAD:] = ik_ref[...]
    pl.semaphore_wait(barrier, len(peers))

    sent = []

    def remote(src, dst, ss, rs, peer):
        return pltpu.make_async_remote_copy(
            src_ref=src, dst_ref=dst, send_sem=ss, recv_sem=rs, device_id=peer, device_id_type=MESH
        )

    def half_ref(sl, half):
        return keys.at[sl, pl.ds(half * HALF, HALF), :]

    count = [0]

    def send_key(sl, half, peer):
        n = count[0]
        count[0] += 1
        cp = remote(half_ref(sl, half), half_ref(sl, half), k_ss.at[n], k_rs.at[sl, half], peer)
        cp.start()
        sent.append(cp)

    def wait_key(sl, half):
        ref = half_ref(sl, half)
        remote(ref, ref, k_ss.at[0], k_rs.at[sl, half], other_core).wait_recv()

    right, left = at_y(1), at_y(NY - 1)
    for half in range(2):
        send_key(s, half, right)
        send_key(s, half, left)
        send_key(s, half, (x_near, x_far)[half])
    for d in FAR_FIRST:
        cp = remote(lq_ref.at[(z + d) % NZ], qrecv.at[d], q_ss.at[d], q_rs.at[d], at_z(d))
        cp.start()
        sent.append(cp)
    for half in range(2):
        send_key(s, half, other_core)
    own_q = pltpu.make_async_copy(lq_ref.at[z], qrecv.at[0], loc_sem)
    own_q.start()

    lane = lax.broadcasted_iota(jnp.int32, (OWN, 128), 1)
    row = lax.broadcasted_iota(jnp.int32, (OWN, 128), 0)
    look = jnp.sum(
        jnp.where(lane == h * OWN + row, jnp.broadcast_to(look_ref[...], (OWN, 128)), 0),
        axis=1, keepdims=True,
    )
    query_pos = s * ROWS + h * OWN + lax.broadcasted_iota(jnp.int32, (OWN, 1), 0)
    query_low = query_pos - look
    iq32 = iq_ref[...].astype(F32)
    iw = iw_ref[...] * FACTOR
    for j in range(IHEADS):
        iqf[j * OWN : (j + 1) * OWN, :] = iq32[:, j * IDIM : (j + 1) * IDIM]
        wbc[j * OWN : (j + 1) * OWN, :] = jnp.broadcast_to(iw[:, j : j + 1], (OWN, CH))
    iqb[...] = iqf[...].astype(BF16)
    iqt[...] = iqf[...].T.astype(BF16)

    def on_y(k, half, going_right):
        yy = (y + NY - k) % NY if going_right else (y + k) % NY
        sl = slot(x_lo, yy, core)
        wait_key(sl, half)
        if k < 3 or (k == 3 and half == (0 if going_right else 1)):
            send_key(sl, half, right if going_right else left)
        send_key(sl, half, (x_near, x_far)[half])
        send_key(sl, half, other_core)

    def on_x(yy):
        sl = slot(1 - x_lo, yy, core)
        for half in range(2):
            wait_key(sl, half)
            send_key(sl, half, other_core)

    for k in range(1, 5):
        if k < 4:
            for half in range(2):
                on_y(k, half, True)
                on_y(k, half, False)
        else:
            on_y(4, 0, True)
            on_y(4, 1, False)
        on_x((y + NY - k + 1) % NY)
        if k > 1:
            on_x((y + k - 1) % NY)
    on_x((y + 4) % NY)

    nrm = norm_ref[pl.ds(pl.multiple_of(z * QROWS, QROWS), QROWS), :] * LOG2E
    lane16 = lax.broadcasted_iota(jnp.int32, (QROWS, 128), 1)
    for pos, d in enumerate(SLABS):
        first = (((z + NZ - d) % NZ) * 2 + x_hi) * LOCAL_HEADS
        for g in range(LOCAL_HEADS):
            col = jnp.sum(jnp.where(lane16 == first + g, nrm, 0.0), axis=1, keepdims=True)
            at = (pos * LOCAL_HEADS + g) * QROWS
            nbc[at : at + QROWS, :] = jnp.broadcast_to(col, (QROWS, CH))

    def build(positions):
        for pos in positions:
            d = SLABS[pos]
            if d:
                remote(qrecv.at[d], qrecv.at[d], q_ss.at[d], q_rs.at[d], at_z(d)).wait_recv()
            else:
                own_q.wait()
            for p in range(LOCAL_HEADS // 2):
                at = (pos * LOCAL_HEADS + 2 * p) * QROWS
                base = 2 * p * KDIM
                qmat[at : at + QROWS, :] = qrecv[d, :, base : base + KPAD]
                odd = qrecv[d, :, base + 512 : base + 512 + KPAD].astype(F32)
                odd = pltpu.roll(odd, KPAD - 64, 1)
                qmat[at + QROWS : at + 2 * QROWS, :] = odd.astype(BF16)

    def mass_of(j, groups):
        kk = keys[pl.ds(2 * j, 2), :, :KPAD].reshape(CH, KPAD)
        total = jnp.zeros((QROWS, CH), F32)
        for q in groups:
            sc = lax.dot_general(
                qmat[q * GROUP : (q + 1) * GROUP, :], kk, (((1,), (1,)), ((), ())),
                preferred_element_type=F32,
            )
            ex = jnp.exp2(sc * (SCORE_SCALE * LOG2E) - nbc[q * GROUP : (q + 1) * GROUP, :])
            total = total + jnp.sum(ex.reshape(GROUP // QROWS, QROWS, CH), axis=0)
        return total.reshape(2, OWN, CH)

    def near(t):
        return (y + NY + (2 * (t % 2) - 1) * ((t + 1) // 2)) % NY

    def mass_early(pieces):
        for xl, t in pieces:
            for half in range(2):
                wait_key(slot(xl, near(t), 1 - core), half)
        totals = [mass_of(xl * NY + near(t), (0, 1)) for xl, t in pieces]
        for (xl, t), total in zip(pieces, totals):
            mpart[xl * NY + near(t)] = total

    def mass_pair(i, carry):
        mass_early(((x_lo, i + 2), (1 - x_lo, i)))
        return carry

    def mass_late(i, carry):
        totals = [mass_of(2 * i + u, (2, 3)) for u in range(2)]
        for u, total in enumerate(totals):
            mpart[2 * i + u] = mpart[2 * i + u] + total
        return carry

    def swap(c):
        return remote(
            mpart.at[pl.ds(4 * c, 4), 1 - x_hi], mrecv.at[pl.ds(4 * c, 4)],
            m_ss.at[c], m_rs.at[c], x_two,
        )

    def visible(j):
        key_pos = j * CH + lax.broadcasted_iota(jnp.int32, (OWN, CH), 1)
        return (key_pos <= query_pos) & (key_pos >= query_low)

    build((0, 1, 2, 3))
    mass_early(((x_lo, 0), (x_lo, 1)))
    lax.fori_loop(0, NY - 2, mass_pair, 0)
    mass_early(((1 - x_lo, NY - 2), (1 - x_lo, NY - 1)))
    build((4, 5, 6, 7))
    for c in range(4):
        lax.fori_loop(2 * c, 2 * c + 2, mass_late, 0)
        cp = swap(c)
        cp.start()
        sent.append(cp)

    def score_step(i, top):
        raws = []
        for u in range(4):
            kk = keys[pl.ds(8 * i + 2 * u, 2), :, KPAD:].reshape(CH, IDIM)
            raws.append(
                lax.dot_general(
                    iqb[...], kk, (((1,), (1,)), ((), ())), preferred_element_type=F32
                )
            )
        for u, raw in enumerate(raws):
            inner[4 * i + u] = raw
            act = jnp.maximum(raw, 0.0) * wbc[...]
            score = jnp.sum(act.reshape(IHEADS, OWN, CH), axis=0)
            score = jnp.where(visible(4 * i + u), score, -jnp.inf)
            pred[4 * i + u] = score
            top = jnp.maximum(top, score)
        return top

    top = lax.fori_loop(0, NCH // 4, score_step, jnp.full((OWN, CH), -jnp.inf, F32))
    top = jnp.max(top, axis=1, keepdims=True)
    p_all = jnp.exp(pred[...] - top[None])
    p_sum = jnp.sum(jnp.sum(p_all, axis=0), axis=1, keepdims=True)
    pred[...] = p_all / p_sum[None]

    for c in range(4):
        swap(c).wait_recv()

    def mass_sum(j, acc):
        m = jnp.where(visible(j), mpart[j, x_hi] + mrecv[j], 0.0)
        mrecv[j] = m
        return acc + m

    mass = lax.fori_loop(0, NCH, mass_sum, jnp.zeros((OWN, CH), F32))
    mass = jnp.sum(mass, axis=1, keepdims=True)

    def r1_copy(j):
        return remote(dkey.at[j, 1 - core], r1recv.at[j], r1_ss.at[j], r1_rs.at[j], other_core)

    def far(t):
        return (4 + (1 - 2 * (t % 2)) * ((t + 1) // 2)) % NY

    def row_of(t):
        return (y + far(t)) % NY

    def y_copy(yy, d):
        return remote(py.at[yy], ry.at[d], y2_ss.at[d], y2_rs.at[d], dev(x_lo, yy, core, z, x_hi))

    def z_copy(part, d):
        return remote(
            pz.at[part, (z + d) % NZ], rz.at[part, d], z2_ss.at[part, d], z2_rs.at[part, d], at_z(d)
        )

    def key_grads(js):
        slopes = []
        for j in js:
            gap = pred[j] - mrecv[j] / mass
            pred[j] = gap
            raw = inner[j].reshape(IHEADS, OWN, CH)
            slope = jnp.where(raw > 0, gap[None] * wbc[...].reshape(IHEADS, OWN, CH), 0.0)
            slopes.append(slope.reshape(IHEADS * OWN, CH).astype(BF16))
        dks = [jnp.dot(iqt[...], slope, preferred_element_type=F32) for slope in slopes]
        for j, slope, dk in zip(js, slopes, dks):
            slp[j] = slope
            dkey[j] = dk.T.reshape(2, ROWS, IDIM)
        for j in js:
            r1_copy(j).start()

    def r1_sum(t):
        yy = row_of(t)
        both = []
        for xl in range(NX_LO):
            j = xl * NY + yy
            r1_copy(j).wait_recv()
            both.append((dkey[j, core] + r1recv[j]).reshape(NZ, 2, OWN, IDIM))
        pz[t // 4, :, t % 4] = jnp.concatenate([b[:, 0] for b in both], axis=1).astype(BF16)
        py[yy] = jnp.concatenate([b[:, 1] for b in both], axis=1).astype(BF16)

    def key_step(t, carry):
        key_grads([xl * NY + row_of(t) for xl in range(NX_LO)])

        @pl.when(t >= 1)
        def _():
            r1_sum(t - 1)
            y_copy(row_of(t - 1), far(t - 1)).start()

        return carry

    def z_start(part):
        for d in FAR_FIRST:
            cp = z_copy(part, d)
            cp.start()
            sent.append(cp)

    lax.fori_loop(0, 5, key_step, 0)
    z_start(0)
    lax.fori_loop(5, NY, key_step, 0)
    r1_sum(NY - 1)
    z_start(1)

    dqa[...] = jnp.zeros_like(dqa)
    dwa[...] = jnp.zeros_like(dwa)

    def own_grad(i, carry):
        dq = jnp.zeros((IHEADS * OWN, IDIM), F32)
        dw = jnp.zeros((IHEADS * OWN, 128), F32)
        for u in range(4):
            j = 4 * i + u
            act = jnp.maximum(inner[j].reshape(IHEADS, OWN, CH), 0.0) * pred[j][None]
            act = act.reshape(IHEADS * OWN, CH)
            dw = dw + (act[:, :128] + act[:, 128:])
            kk = keys[pl.ds(2 * j, 2), :, KPAD:].reshape(CH, IDIM)
            dq = dq + jnp.dot(slp[j], kk, preferred_element_type=F32)
        dqa[...] += dq
        dwa[...] += dw
        return carry

    lax.fori_loop(0, NCH // 4, own_grad, 0)
    lane_w = lax.broadcasted_iota(jnp.int32, (OWN, 128), 1)
    gw = jnp.zeros((OWN, 128), F32)
    for j in range(IHEADS):
        out_ref[:, j * IDIM : (j + 1) * IDIM] = dqa[j * OWN : (j + 1) * OWN, :]
        col = jnp.sum(dwa[j * OWN : (j + 1) * OWN, :], axis=1, keepdims=True)
        gw = jnp.where(lane_w == j, jnp.broadcast_to(col, (OWN, 128)), gw)
    out_ref[:, OUT_W : OUT_W + 128] = gw * FACTOR

    az, ay = [pz[0, z].astype(F32), pz[1, z].astype(F32)], py[y].astype(F32)
    for part in range(2):
        for d in (1, 7, 2, 6, 3, 5, 4):
            z_copy(part, d).wait_recv()
            az[part] = az[part] + rz[part, d].astype(F32)
    for d in (1, 7, 2, 6, 3, 5, 4):
        remote(py.at[d], ry.at[d], y2_ss.at[d], y2_rs.at[d], at_y(d)).wait_recv()
        ay = ay + ry[d].astype(F32)
    sz[:4] = az[0].reshape(NY // 2, NX_LO, OWN, IDIM)
    sz[4:] = az[1].reshape(NY // 2, NX_LO, OWN, IDIM)
    sy[...] = ay.reshape(NZ, NX_LO, OWN, IDIM)
    for t, d in enumerate(FAR_FIRST):
        for cp in (
            remote(sz.at[t], r3z.at[d], y3_ss.at[d], y3_rs.at[d], at_y(d)),
            remote(sy.at[(z + d) % NZ], r3y.at[d], z3_ss.at[d], z3_rs.at[d], at_z(d)),
        ):
            cp.start()
            sent.append(cp)
    t0, t1 = sz[NY - 1], sy[z]
    for d in (1, 7, 2, 6, 3, 5, 4):
        remote(sz.at[d], r3z.at[d], y3_ss.at[d], y3_rs.at[d], at_y(d)).wait_recv()
        remote(sy.at[d], r3y.at[d], z3_ss.at[d], z3_rs.at[d], at_z(d)).wait_recv()
        t0 = t0 + r3z[d]
        t1 = t1 + r3y[d]
    tx[0] = t0
    tx[1] = t1
    last = []
    for n, (peer, xh, xl) in enumerate(
        ((x_near, x_hi, 1 - x_lo), (x_far, 1 - x_hi, 1 - x_lo), (x_two, 1 - x_hi, x_lo))
    ):
        cp = remote(tx.at[xh, xl], r4.at[n], x4_ss.at[n], x4_rs.at[n], peer)
        cp.start()
        sent.append(cp)
        last.append(cp)
    out = tx[x_hi, x_lo]
    for n, cp in enumerate(last):
        cp.wait_recv()
        out = out + r4[n]
    out_ref[:, OUT_W + 128 :] = out

    for cp in sent:
        cp.wait_send()

    def r1_done(j, carry):
        r1_copy(j).wait_send()
        return carry

    lax.fori_loop(0, NCH, r1_done, 0)

    def y_done(t, carry):
        y_copy(row_of(t), far(t)).wait_send()
        return carry

    lax.fori_loop(0, NY - 1, y_done, 0)


def split_kernel(all_ref, gq_ref, gw_ref, gk_ref):
    gq_ref[...] = all_ref[:, :OUT_W]
    gw_ref[...] = all_ref[:, OUT_W : OUT_W + IHEADS]
    gk_ref[...] = all_ref[:, OUT_W + 128 :]


def per_device(lat_query, lat_keys, normalizer, lookback, index_query, index_keys, index_weight):
    vmem = pl.BlockSpec(memory_space=pltpu.VMEM)
    dma = pltpu.SemaphoreType.DMA
    together = pl.pallas_call(
        kernel,
        out_shape=jax.ShapeDtypeStruct((OWN, OUT_W + 256), F32),
        in_specs=[pl.BlockSpec(memory_space=pl.ANY)] + [vmem] * 6,
        out_specs=vmem,
        scratch_shapes=[
            pltpu.VMEM((NZ, QROWS, LOCAL_HEADS * KDIM), BF16),
            pltpu.VMEM((NZ * LOCAL_HEADS * QROWS, KPAD), BF16),
            pltpu.VMEM((SLOTS, ROWS, KPAD + IDIM), BF16),
            pltpu.VMEM((NZ * LOCAL_HEADS * QROWS, CH), F32),
            pltpu.VMEM((IHEADS * OWN, CH), F32),
            pltpu.VMEM((IHEADS * OWN, IDIM), F32),
            pltpu.VMEM((IHEADS * OWN, IDIM), BF16),
            pltpu.VMEM((IDIM, IHEADS * OWN), BF16),
            pltpu.VMEM((NCH, IHEADS * OWN, CH), F32),
            pltpu.VMEM((NCH, OWN, CH), F32),
            pltpu.VMEM((NCH, 2, OWN, CH), F32),
            pltpu.VMEM((NCH, OWN, CH), F32),
            pltpu.VMEM((IHEADS * OWN, IDIM), F32),
            pltpu.VMEM((IHEADS * OWN, 128), F32),
            pltpu.VMEM((NCH, IHEADS * OWN, CH), BF16),
            pltpu.VMEM((NCH, 2, ROWS, IDIM), F32),
            pltpu.VMEM((NCH, ROWS, IDIM), F32),
            pltpu.VMEM((2, NZ, NY // 2, NX_LO * OWN, IDIM), BF16),
            pltpu.VMEM((NY, NZ, NX_LO * OWN, IDIM), BF16),
            pltpu.VMEM((2, NZ, NY // 2, NX_LO * OWN, IDIM), BF16),
            pltpu.VMEM((NY, NZ, NX_LO * OWN, IDIM), BF16),
            pltpu.VMEM((NY, NX_LO, OWN, IDIM), F32),
            pltpu.VMEM((NZ, NX_LO, OWN, IDIM), F32),
            pltpu.VMEM((NY, NX_LO, OWN, IDIM), F32),
            pltpu.VMEM((NZ, NX_LO, OWN, IDIM), F32),
            pltpu.VMEM((NX_HI, NX_LO, OWN, IDIM), F32),
            pltpu.VMEM((3, OWN, IDIM), F32),
            dma((NZ,)), dma((NZ,)), dma((64,)), dma((SLOTS, 2)), dma((4,)), dma((4,)),
            dma((NCH,)), dma((NCH,)),
            dma((2, NZ)), dma((2, NZ)), dma((NY,)), dma((NY,)),
            dma((NZ,)), dma((NZ,)), dma((NY,)), dma((NY,)),
            dma((3,)), dma((3,)), dma,
        ],
        compiler_params=pltpu.CompilerParams(
            collective_id=0, has_side_effects=True, vmem_limit_bytes=56 << 20
        ),
    )(
        lat_query.reshape(NZ, QROWS, LOCAL_HEADS * KDIM),
        lat_keys.T,
        normalizer,
        lookback.reshape(1, ROWS),
        index_query,
        index_keys,
        index_weight,
    )
    return pl.pallas_call(
        split_kernel,
        out_shape=(
            jax.ShapeDtypeStruct((OWN, OUT_W), F32),
            jax.ShapeDtypeStruct((OWN, IHEADS), F32),
            jax.ShapeDtypeStruct((OWN, IDIM), F32),
        ),
        in_specs=[vmem],
        out_specs=(vmem, vmem, vmem),
    )(together)


def solution(mesh):
    return jax.shard_map(
        per_device,
        mesh=mesh,
        in_specs=(
            P("seq", "head"),
            P("seq", None),
            P("seq", None),
            P("seq"),
            P(("seq", "head"), None),
            P("seq", None),
            P(("seq", "head"), None),
        ),
        out_specs=(P(("seq", "head"), None), P(("seq", "head"), None), P(("seq", "head"), None)),
        check_vma=False,
    )
```

```python
import functools
import math

import jax
import jax.numpy as jnp
from jax import lax
from jax.experimental import pallas as pl
from jax.experimental.pallas import tpu as pltpu
from jax.sharding import PartitionSpec as P

F32 = jnp.float32
BF16 = jnp.bfloat16
KDIM = 576
KPAD = 640
IDIM = 128
IHEADS = 64
NX_LO, NY, NCORE = 2, 8, 2
NZ, NX_HI = 8, 2
SLOTS = NX_LO * NY * NCORE
ROWS = 128
HALF = ROWS // 2
OWN = 8
QROWS = 16
LOCAL_HEADS = 8
CH = 256
NCH = SLOTS * ROWS // CH
LOG2E = math.log2(math.e)
SCORE_SCALE = KDIM ** (-0.5)
FACTOR = IDIM ** (-0.5)
MESH = pl.DeviceIdType.MESH
SLABS = (0, 4, 3, 5, 2, 6, 1, 7)
FAR_FIRST = (4, 3, 5, 2, 6, 1, 7)
GROUP = 256
OUT_W = IHEADS * IDIM


def kernel(
    lq_ref, lk_ref, norm_ref, look_ref, iq_ref, ik_ref, iw_ref,
    out_ref,
    qrecv, qmat, keys, nbc, wbc, iqf, iqb, iqt, inner, pred, mpart, mrecv,
    dqa, dwa, slp, dkey, r1recv, pz, py, rz, ry, sz, sy, r3z, r3y, tx, r4,
    q_ss, q_rs, k_ss, k_rs, m_ss, m_rs, r1_ss, r1_rs,
    z2_ss, z2_rs, y2_ss, y2_rs, z3_ss, z3_rs, y3_ss, y3_rs, x4_ss, x4_rs, loc_sem,
):
    s = lax.axis_index("seq")
    h = lax.axis_index("head")
    core = s % 2
    y = (s // 2) % NY
    x_lo = s // (2 * NY)
    x_hi = h % 2
    z = h // 2

    def slot(xl, yy, cc):
        return (xl * NY + yy) * 2 + cc

    def dev(xl, yy, cc, zz, xh):
        return (slot(xl, yy, cc), zz * 2 + xh)

    def at_z(d):
        return dev(x_lo, y, core, (z + d) % NZ, x_hi)

    def at_y(d):
        return dev(x_lo, (y + d) % NY, core, z, x_hi)

    other_core = dev(x_lo, y, 1 - core, z, x_hi)
    x_near = dev(1 - x_lo, y, core, z, x_hi)
    x_far = dev(1 - x_lo, y, core, z, 1 - x_hi)
    x_two = dev(x_lo, y, core, z, 1 - x_hi)

    barrier = pltpu.get_barrier_semaphore()
    peers = [at_z(d) for d in range(1, NZ)] + [at_y(d) for d in range(1, NY)]
    peers += [other_core, x_near, x_far, x_two]
    for peer in peers:
        pl.semaphore_signal(barrier, inc=1, device_id=peer, device_id_type=MESH)

    for i in range(4):
        part = lk_ref[i * 128 : (i + 1) * 128, :].astype(F32)
        keys[s, :, i * 128 : (i + 1) * 128] = part.T.astype(BF16)
    part = jnp.concatenate(
        [lk_ref[512:KDIM, :].astype(F32), jnp.zeros((KPAD - KDIM, ROWS), F32)], axis=0
    )
    keys[s, :, 512:KPAD] = part.T.astype(BF16)
    keys[s, :, KPAD:] = ik_ref[...]
    pl.semaphore_wait(barrier, len(peers))

    sent = []

    def remote(src, dst, ss, rs, peer):
        return pltpu.make_async_remote_copy(
            src_ref=src, dst_ref=dst, send_sem=ss, recv_sem=rs, device_id=peer, device_id_type=MESH
        )

    def half_ref(sl, half):
        return keys.at[sl, pl.ds(half * HALF, HALF), :]

    count = [0]

    def send_key(sl, half, peer):
        n = count[0]
        count[0] += 1
        cp = remote(half_ref(sl, half), half_ref(sl, half), k_ss.at[n], k_rs.at[sl, half], peer)
        cp.start()
        sent.append(cp)

    def wait_key(sl, half):
        ref = half_ref(sl, half)
        remote(ref, ref, k_ss.at[0], k_rs.at[sl, half], other_core).wait_recv()

    right, left = at_y(1), at_y(NY - 1)
    for d in FAR_FIRST:
        cp = remote(lq_ref.at[(z + d) % NZ], qrecv.at[d], q_ss.at[d], q_rs.at[d], at_z(d))
        cp.start()
        sent.append(cp)
    for half in range(2):
        send_key(s, half, right)
        send_key(s, half, left)
        send_key(s, half, (x_near, x_far)[half])
    for half in range(2):
        send_key(s, half, other_core)
    own_q = pltpu.make_async_copy(lq_ref.at[z], qrecv.at[0], loc_sem)
    own_q.start()

    lane = lax.broadcasted_iota(jnp.int32, (OWN, 128), 1)
    row = lax.broadcasted_iota(jnp.int32, (OWN, 128), 0)
    look = jnp.sum(
        jnp.where(lane == h * OWN + row, jnp.broadcast_to(look_ref[...], (OWN, 128)), 0),
        axis=1, keepdims=True,
    )
    query_pos = s * ROWS + h * OWN + lax.broadcasted_iota(jnp.int32, (OWN, 1), 0)
    query_low = query_pos - look
    iq32 = iq_ref[...].astype(F32)
    iw = iw_ref[...] * FACTOR
    for j in range(IHEADS):
        iqf[j * OWN : (j + 1) * OWN, :] = iq32[:, j * IDIM : (j + 1) * IDIM]
        wbc[j * OWN : (j + 1) * OWN, :] = jnp.broadcast_to(iw[:, j : j + 1], (OWN, CH))
    iqb[...] = iqf[...].astype(BF16)
    iqt[...] = iqf[...].T.astype(BF16)

    nrm = norm_ref[pl.ds(pl.multiple_of(z * QROWS, QROWS), QROWS), :] * LOG2E
    lane16 = lax.broadcasted_iota(jnp.int32, (QROWS, 128), 1)
    for pos, d in enumerate(SLABS):
        first = (((z + NZ - d) % NZ) * 2 + x_hi) * LOCAL_HEADS
        for g in range(LOCAL_HEADS):
            col = jnp.sum(jnp.where(lane16 == first + g, nrm, 0.0), axis=1, keepdims=True)
            at = (pos * LOCAL_HEADS + g) * QROWS
            nbc[at : at + QROWS, :] = jnp.broadcast_to(col, (QROWS, CH))

    def build(positions):
        for pos in positions:
            d = SLABS[pos]
            if d:
                remote(qrecv.at[d], qrecv.at[d], q_ss.at[d], q_rs.at[d], at_z(d)).wait_recv()
            else:
                own_q.wait()
            for p in range(LOCAL_HEADS // 2):
                at = (pos * LOCAL_HEADS + 2 * p) * QROWS
                base = 2 * p * KDIM
                qmat[at : at + QROWS, :] = qrecv[d, :, base : base + KPAD]
                odd = qrecv[d, :, base + 512 : base + 512 + KPAD].astype(F32)
                odd = pltpu.roll(odd, KPAD - 64, 1)
                qmat[at + QROWS : at + 2 * QROWS, :] = odd.astype(BF16)

    build((0,))

    def on_y(k, half, going_right):
        yy = (y + NY - k) % NY if going_right else (y + k) % NY
        sl = slot(x_lo, yy, core)
        wait_key(sl, half)
        if k < 3 or (k == 3 and half == (0 if going_right else 1)):
            send_key(sl, half, right if going_right else left)
        send_key(sl, half, (x_near, x_far)[half])
        send_key(sl, half, other_core)

    def on_x(yy):
        sl = slot(1 - x_lo, yy, core)
        for half in range(2):
            wait_key(sl, half)
            send_key(sl, half, other_core)

    for k in range(1, 5):
        if k < 4:
            for half in range(2):
                on_y(k, half, True)
                on_y(k, half, False)
        else:
            on_y(4, 0, True)
            on_y(4, 1, False)
        on_x((y + NY - k + 1) % NY)
        if k > 1:
            on_x((y + k - 1) % NY)
    on_x((y + 4) % NY)

    def mass_of(j, groups):
        kk = keys[pl.ds(2 * j, 2), :, :KPAD].reshape(CH, KPAD)
        total = jnp.zeros((QROWS, CH), F32)
        for q in groups:
            sc = lax.dot_general(
                qmat[q * GROUP : (q + 1) * GROUP, :], kk, (((1,), (1,)), ((), ())),
                preferred_element_type=F32,
            )
            ex = jnp.exp2(sc * (SCORE_SCALE * LOG2E) - nbc[q * GROUP : (q + 1) * GROUP, :])
            total = total + jnp.sum(ex.reshape(GROUP // QROWS, QROWS, CH), axis=0)
        return total.reshape(2, OWN, CH)

    def near(t):
        return (y + NY + (2 * (t % 2) - 1) * ((t + 1) // 2)) % NY

    def mass_early(pieces):
        for xl, t in pieces:
            for half in range(2):
                wait_key(slot(xl, near(t), 1 - core), half)
        totals = [mass_of(xl * NY + near(t), (0, 1)) for xl, t in pieces]
        for (xl, t), total in zip(pieces, totals):
            mpart[xl * NY + near(t)] = total

    def mass_pair(i, carry):
        mass_early(((x_lo, i + 2), (1 - x_lo, i)))
        return carry

    def mass_late(group, chunks):
        def step(i, carry):
            totals = [mass_of(chunks * i + u, (group,)) for u in range(chunks)]
            for u, total in enumerate(totals):
                mpart[chunks * i + u] = mpart[chunks * i + u] + total
            return carry

        return step

    def swap(c):
        return remote(
            mpart.at[pl.ds(4 * c, 4), 1 - x_hi], mrecv.at[pl.ds(4 * c, 4)],
            m_ss.at[c], m_rs.at[c], x_two,
        )

    def visible(j):
        key_pos = j * CH + lax.broadcasted_iota(jnp.int32, (OWN, CH), 1)
        return (key_pos <= query_pos) & (key_pos >= query_low)

    build((1, 2, 3))
    mass_early(((x_lo, 0), (x_lo, 1)))
    lax.fori_loop(0, NY - 2, mass_pair, 0)
    mass_early(((1 - x_lo, NY - 2), (1 - x_lo, NY - 1)))
    build((4, 5))
    lax.fori_loop(0, NCH // 4, mass_late(2, 4), 0)
    build((6, 7))
    for c in range(4):
        mass_late(3, 4)(c, 0)
        cp = swap(c)
        cp.start()
        sent.append(cp)

    def score_step(i, top):
        raws = []
        for u in range(4):
            kk = keys[pl.ds(8 * i + 2 * u, 2), :, KPAD:].reshape(CH, IDIM)
            raws.append(
                lax.dot_general(
                    iqb[...], kk, (((1,), (1,)), ((), ())), preferred_element_type=F32
                )
            )
        for u, raw in enumerate(raws):
            inner[4 * i + u] = raw
            act = jnp.maximum(raw, 0.0) * wbc[...]
            score = jnp.sum(act.reshape(IHEADS, OWN, CH), axis=0)
            score = jnp.where(visible(4 * i + u), score, -jnp.inf)
            pred[4 * i + u] = score
            top = jnp.maximum(top, score)
        return top

    top = lax.fori_loop(0, NCH // 4, score_step, jnp.full((OWN, CH), -jnp.inf, F32))
    top = jnp.max(top, axis=1, keepdims=True)
    p_all = jnp.exp(pred[...] - top[None])
    p_sum = jnp.sum(jnp.sum(p_all, axis=0), axis=1, keepdims=True)
    pred[...] = p_all / p_sum[None]

    for c in range(4):
        swap(c).wait_recv()

    def mass_sum(j, acc):
        m = jnp.where(visible(j), mpart[j, x_hi] + mrecv[j], 0.0)
        mrecv[j] = m
        return acc + m

    mass = lax.fori_loop(0, NCH, mass_sum, jnp.zeros((OWN, CH), F32))
    mass = jnp.sum(mass, axis=1, keepdims=True)

    def r1_copy(j):
        return remote(dkey.at[j, 1 - core], r1recv.at[j], r1_ss.at[j], r1_rs.at[j], other_core)

    def far(t):
        return (4 + (1 - 2 * (t % 2)) * ((t + 1) // 2)) % NY

    def row_of(t):
        return (y + far(t)) % NY

    def y_copy(yy, d):
        return remote(py.at[yy], ry.at[d], y2_ss.at[d], y2_rs.at[d], dev(x_lo, yy, core, z, x_hi))

    def z_copy(part, d):
        return remote(
            pz.at[part, (z + d) % NZ], rz.at[part, d], z2_ss.at[part, d], z2_rs.at[part, d], at_z(d)
        )

    def key_grads(js):
        slopes = []
        for j in js:
            gap = pred[j] - mrecv[j] / mass
            pred[j] = gap
            raw = inner[j].reshape(IHEADS, OWN, CH)
            slope = jnp.where(raw > 0, gap[None] * wbc[...].reshape(IHEADS, OWN, CH), 0.0)
            slopes.append(slope.reshape(IHEADS * OWN, CH).astype(BF16))
        dks = [jnp.dot(iqt[...], slope, preferred_element_type=F32) for slope in slopes]
        for j, slope, dk in zip(js, slopes, dks):
            slp[j] = slope
            dkey[j] = dk.T.reshape(2, ROWS, IDIM)
        for j in js:
            r1_copy(j).start()

    def r1_sum(t):
        yy = row_of(t)
        both = []
        for xl in range(NX_LO):
            j = xl * NY + yy
            r1_copy(j).wait_recv()
            both.append((dkey[j, core] + r1recv[j]).reshape(NZ, 2, OWN, IDIM))
        pz[t // 2, :, t % 2] = jnp.concatenate([b[:, 0] for b in both], axis=1).astype(BF16)
        py[yy] = jnp.concatenate([b[:, 1] for b in both], axis=1).astype(BF16)

    def reduce_step(i, own_last):
        for u in range(2):
            t = 2 * i + u
            r1_sum(t)
            if not (own_last and u):
                y_copy(row_of(t), far(t)).start()
        for d in FAR_FIRST:
            z_copy(i, d).start()

    def key_step(i, carry):
        key_grads([xl * NY + row_of(2 * i + u) for u in range(2) for xl in range(NX_LO)])

        @pl.when(i >= 1)
        def _():
            reduce_step(i - 1, False)

        return carry

    lax.fori_loop(0, NY // 2, key_step, 0)
    reduce_step(NY // 2 - 1, True)

    dqa[...] = jnp.zeros_like(dqa)
    dwa[...] = jnp.zeros_like(dwa)

    def own_grad(i, carry):
        dq = jnp.zeros((IHEADS * OWN, IDIM), F32)
        dw = jnp.zeros((IHEADS * OWN, 128), F32)
        for u in range(4):
            j = 4 * i + u
            act = jnp.maximum(inner[j].reshape(IHEADS, OWN, CH), 0.0) * pred[j][None]
            act = act.reshape(IHEADS * OWN, CH)
            dw = dw + (act[:, :128] + act[:, 128:])
            kk = keys[pl.ds(2 * j, 2), :, KPAD:].reshape(CH, IDIM)
            dq = dq + jnp.dot(slp[j], kk, preferred_element_type=F32)
        dqa[...] += dq
        dwa[...] += dw
        return carry

    lax.fori_loop(0, NCH // 4, own_grad, 0)
    lane_w = lax.broadcasted_iota(jnp.int32, (OWN, 128), 1)
    gw = jnp.zeros((OWN, 128), F32)
    for j in range(IHEADS):
        out_ref[:, j * IDIM : (j + 1) * IDIM] = dqa[j * OWN : (j + 1) * OWN, :]
        col = jnp.sum(dwa[j * OWN : (j + 1) * OWN, :], axis=1, keepdims=True)
        gw = jnp.where(lane_w == j, jnp.broadcast_to(col, (OWN, 128)), gw)
    out_ref[:, OUT_W : OUT_W + 128] = gw * FACTOR

    ay = py[y].astype(F32)
    for d in (1, 7, 2, 6, 3, 5, 4):
        remote(py.at[d], ry.at[d], y2_ss.at[d], y2_rs.at[d], at_y(d)).wait_recv()
        ay = ay + ry[d].astype(F32)
    sy[...] = ay.reshape(NZ, NX_LO, OWN, IDIM)
    for d in FAR_FIRST:
        cp = remote(sy.at[(z + d) % NZ], r3y.at[d], z3_ss.at[d], z3_rs.at[d], at_z(d))
        cp.start()
        sent.append(cp)
    for part in range(NY // 2):
        az = pz[part, z].astype(F32)
        for d in (1, 7, 2, 6, 3, 5, 4):
            z_copy(part, d).wait_recv()
            az = az + rz[part, d].astype(F32)
        sz[2 * part : 2 * part + 2] = az.reshape(2, NX_LO, OWN, IDIM)
        for u in range(2):
            t = 2 * part + u
            if t == NY - 1:
                break
            d = FAR_FIRST[t]
            cp = remote(sz.at[t], r3z.at[d], y3_ss.at[d], y3_rs.at[d], at_y(d))
            cp.start()
            sent.append(cp)
    t0, t1 = sz[NY - 1], sy[z]
    for d in (1, 7, 2, 6, 3, 5, 4):
        remote(sz.at[d], r3z.at[d], y3_ss.at[d], y3_rs.at[d], at_y(d)).wait_recv()
        remote(sy.at[d], r3y.at[d], z3_ss.at[d], z3_rs.at[d], at_z(d)).wait_recv()
        t0 = t0 + r3z[d]
        t1 = t1 + r3y[d]
    tx[0] = t0
    tx[1] = t1
    last = []
    for n, (peer, xh, xl) in enumerate(
        ((x_near, x_hi, 1 - x_lo), (x_far, 1 - x_hi, 1 - x_lo), (x_two, 1 - x_hi, x_lo))
    ):
        cp = remote(tx.at[xh, xl], r4.at[n], x4_ss.at[n], x4_rs.at[n], peer)
        cp.start()
        sent.append(cp)
        last.append(cp)
    out = tx[x_hi, x_lo]
    for n, cp in enumerate(last):
        cp.wait_recv()
        out = out + r4[n]
    out_ref[:, OUT_W + 128 :] = out

    for cp in sent:
        cp.wait_send()

    def r1_done(j, carry):
        r1_copy(j).wait_send()
        return carry

    lax.fori_loop(0, NCH, r1_done, 0)

    def y_done(t, carry):
        y_copy(row_of(t), far(t)).wait_send()
        return carry

    lax.fori_loop(0, NY - 1, y_done, 0)

    def z_done(part, carry):
        for d in FAR_FIRST:
            z_copy(part, d).wait_send()
        return carry

    lax.fori_loop(0, NY // 2, z_done, 0)


def split_kernel(all_ref, gq_ref, gw_ref, gk_ref):
    gq_ref[...] = all_ref[:, :OUT_W]
    gw_ref[...] = all_ref[:, OUT_W : OUT_W + IHEADS]
    gk_ref[...] = all_ref[:, OUT_W + 128 :]


def per_device(lat_query, lat_keys, normalizer, lookback, index_query, index_keys, index_weight):
    vmem = pl.BlockSpec(memory_space=pltpu.VMEM)
    dma = pltpu.SemaphoreType.DMA
    together = pl.pallas_call(
        kernel,
        out_shape=jax.ShapeDtypeStruct((OWN, OUT_W + 256), F32),
        in_specs=[pl.BlockSpec(memory_space=pl.ANY)] + [vmem] * 6,
        out_specs=vmem,
        scratch_shapes=[
            pltpu.VMEM((NZ, QROWS, LOCAL_HEADS * KDIM), BF16),
            pltpu.VMEM((NZ * LOCAL_HEADS * QROWS, KPAD), BF16),
            pltpu.VMEM((SLOTS, ROWS, KPAD + IDIM), BF16),
            pltpu.VMEM((NZ * LOCAL_HEADS * QROWS, CH), F32),
            pltpu.VMEM((IHEADS * OWN, CH), F32),
            pltpu.VMEM((IHEADS * OWN, IDIM), F32),
            pltpu.VMEM((IHEADS * OWN, IDIM), BF16),
            pltpu.VMEM((IDIM, IHEADS * OWN), BF16),
            pltpu.VMEM((NCH, IHEADS * OWN, CH), F32),
            pltpu.VMEM((NCH, OWN, CH), F32),
            pltpu.VMEM((NCH, 2, OWN, CH), F32),
            pltpu.VMEM((NCH, OWN, CH), F32),
            pltpu.VMEM((IHEADS * OWN, IDIM), F32),
            pltpu.VMEM((IHEADS * OWN, 128), F32),
            pltpu.VMEM((NCH, IHEADS * OWN, CH), BF16),
            pltpu.VMEM((NCH, 2, ROWS, IDIM), F32),
            pltpu.VMEM((NCH, ROWS, IDIM), F32),
            pltpu.VMEM((NY // 2, NZ, 2, NX_LO * OWN, IDIM), BF16),
            pltpu.VMEM((NY, NZ, NX_LO * OWN, IDIM), BF16),
            pltpu.VMEM((NY // 2, NZ, 2, NX_LO * OWN, IDIM), BF16),
            pltpu.VMEM((NY, NZ, NX_LO * OWN, IDIM), BF16),
            pltpu.VMEM((NY, NX_LO, OWN, IDIM), F32),
            pltpu.VMEM((NZ, NX_LO, OWN, IDIM), F32),
            pltpu.VMEM((NY, NX_LO, OWN, IDIM), F32),
            pltpu.VMEM((NZ, NX_LO, OWN, IDIM), F32),
            pltpu.VMEM((NX_HI, NX_LO, OWN, IDIM), F32),
            pltpu.VMEM((3, OWN, IDIM), F32),
            dma((NZ,)), dma((NZ,)), dma((64,)), dma((SLOTS, 2)), dma((4,)), dma((4,)),
            dma((NCH,)), dma((NCH,)),
            dma((NY // 2, NZ)), dma((NY // 2, NZ)), dma((NY,)), dma((NY,)),
            dma((NZ,)), dma((NZ,)), dma((NY,)), dma((NY,)),
            dma((3,)), dma((3,)), dma,
        ],
        compiler_params=pltpu.CompilerParams(
            collective_id=0, has_side_effects=True, vmem_limit_bytes=56 << 20
        ),
    )(
        lat_query.reshape(NZ, QROWS, LOCAL_HEADS * KDIM),
        lat_keys.T,
        normalizer,
        lookback.reshape(1, ROWS),
        index_query,
        index_keys,
        index_weight,
    )
    return pl.pallas_call(
        split_kernel,
        out_shape=(
            jax.ShapeDtypeStruct((OWN, OUT_W), F32),
            jax.ShapeDtypeStruct((OWN, IHEADS), F32),
            jax.ShapeDtypeStruct((OWN, IDIM), F32),
        ),
        in_specs=[vmem],
        out_specs=(vmem, vmem, vmem),
    )(together)


def solution(mesh):
    return jax.shard_map(
        per_device,
        mesh=mesh,
        in_specs=(
            P("seq", "head"),
            P("seq", None),
            P("seq", None),
            P("seq"),
            P(("seq", "head"), None),
            P("seq", None),
            P(("seq", "head"), None),
        ),
        out_specs=(P(("seq", "head"), None), P(("seq", "head"), None), P(("seq", "head"), None)),
        check_vma=False,
    )
```
